256 devices in a mesh: grp: 8 (over y, x_lo), seq: 32 (over x_hi, z, core).
Axes of the slice: x: 4 (x_hi: 2, x_lo: 2; x = x_hi * 2 + x_lo), y: 4, z: 8, core: 2. Of those that a mesh axis runs over, the one named last changes fastest.
Arguments:
- queries: bfloat16 [16, 1024, 8192], P('grp', 'seq'), parts along dimension 0, may hold values from -400 to 400
- stretch_keys: bfloat16 [16, 1024, 1024], P('grp', 'seq'), parts along dimension 0, may hold values from -6 to 6
- stretch_values: bfloat16 [16, 1024, 1024], P('grp', 'seq'), parts along dimension 0, may hold values from -6 to 6
- cache_keys: bfloat16 [16, 2048, 1024], P('grp', 'seq'), parts along dimension 0, may hold values from -6 to 6
- cache_values: bfloat16 [16, 2048, 1024], P('grp', 'seq'), parts along dimension 0, may hold values from -6 to 6
- prefix_len: int32 [16], P('grp'), parts along dimension 0, may hold values from 16 to 2048, as said below
Outputs:
- attention: bfloat16 [16, 1024, 8192], P('grp', 'seq'), parts along dimension 0
- prefix_bounds: bfloat16 [16, 128, 2048], P('grp', 'seq'), parts along dimension 0
- stretch_bounds: bfloat16 [16, 64, 2048], P('grp', 'seq'), parts along dimension 0
The draws below stay inside these ranges and needn't reach their ends.
There are 8 independent parts, one for each index of `grp`. The reference program is written for one: setup_inputs(seed, part) draws one part's arguments, and reference() takes and returns one part's arrays. A program takes and returns all parts, laid end to end along the dimension named above; each array names one. Nothing has to cross between parts.
Inputs may be any that keep to these rules, and one draw needn't show every extreme that they name: `prefix_len`: multiples of 16; some sequence of every group has 2048.
All inputs are finite; a program needn't handle non-finite values.
Results may differ from the reference program's by a relative error of at most 0.006.
Values may be sent and summed in bfloat16 or wider, within the bound.
A program may use at most 128 MiB of HBM per device.

```python
import math
import jax
import jax.numpy as jnp
from jax import lax

HQ = 64
HK = 8
DH = 128
PAGE = 16
SEQS = 2
STRETCH = 1024
PREFIX = 2048


def key_field(base):
    field_values = jnp.clip(jax.random.normal(jax.random.fold_in(base, 11), (SEQS, STRETCH, HK * DH), jnp.float32), -6.0, 6.0)
    return field_values


def draw_stretch_keys(key, part):
    return key_field(key).astype(jnp.bfloat16)


def draw_queries(key, part):
    field_values = jnp.clip(jax.random.normal(jax.random.fold_in(key, 12), (SEQS, STRETCH, HQ * DH), jnp.float32), -6.0, 6.0)
    return field_values.astype(jnp.bfloat16)


def draw_prefix_len(key, part):
    page_count = jax.random.randint(jax.random.fold_in(key, 21), (SEQS,), 1, PREFIX // PAGE + 1)
    full_seq = jax.random.randint(jax.random.fold_in(key, 22), (), 0, SEQS)
    page_count = jnp.where(jnp.arange(SEQS) == full_seq, PREFIX // PAGE, page_count)
    return (page_count * PAGE).astype(jnp.int32)


def steps_of(rng, dims, shards, smallest, high):
    loudness = 1.0
    for dim, blocks in shards:
        steps = jax.random.uniform(jax.random.fold_in(jax.random.fold_in(rng, 6), dim), (blocks,), jnp.float32, smallest / len(shards), high / len(shards))
        loudness = loudness * jnp.repeat(jnp.exp(steps), dims[dim] // blocks).reshape((-1,) + (1,) * (len(dims) - 1 - dim))
    return loudness


def scatter_about(stream_key, extent, spread, most, split=(), kind=jnp.bfloat16):
    factor_of = steps_of(stream_key, extent, split, -0.22, 0.18) if split else 1.0
    array = jax.random.normal(stream_key, extent, jnp.float32) * spread * factor_of
    return jnp.minimum(jnp.maximum(array, -most), most).astype(kind)


def setup_inputs(seed: int = 0, part: int = 0) -> dict:
    keys = jax.random.split(jax.random.key(seed), 7)
    part_splits = jax.random.split(jax.random.fold_in(keys[6], part), 7)
    queries = draw_queries(jax.random.fold_in(jax.random.fold_in(keys[6], part), 71), part)
    stretch_keys = draw_stretch_keys(jax.random.fold_in(jax.random.fold_in(keys[6], part), 71), part)
    stretch_values = scatter_about(part_splits[2], (SEQS, STRETCH, HK * DH), 1.0, 6.0, ((1, 32),))
    cache_keys = scatter_about(part_splits[3], (SEQS, PREFIX, HK * DH), 1.0, 6.0, ((1, 32),))
    cache_values = scatter_about(part_splits[4], (SEQS, PREFIX, HK * DH), 1.0, 6.0, ((1, 32),))
    prefix_len = draw_prefix_len(jax.random.fold_in(jax.random.fold_in(keys[6], part), 71), part)
    return dict(queries=queries, stretch_keys=stretch_keys, stretch_values=stretch_values, cache_keys=cache_keys, cache_values=cache_values, prefix_len=prefix_len)


def page_bounds(key_rows, live_pages):
    shaped = key_rows.reshape(key_rows.shape[0] // PAGE, PAGE, key_rows.shape[1])
    joined = jnp.concatenate([lax.optimization_barrier(jnp.min(shaped, axis=1)), lax.optimization_barrier(jnp.max(shaped, axis=1))], axis=1)
    return jnp.where(live_pages[:, None], joined, jnp.zeros_like(joined))

def reference(queries, stretch_keys, stretch_values, cache_keys, cache_values, prefix_len):
    group = HQ // HK
    factor = 1.0 / math.sqrt(DH)
    block = math.gcd(STRETCH, 256)
    key_index = jnp.arange(PREFIX + STRETCH, dtype=jnp.int32)

    def one_sequence(operands):
        query_rows, new_keys, new_values, old_keys, old_values, length = operands
        key_rows = jnp.concatenate([old_keys, new_keys], axis=0).astype(jnp.float32).reshape(PREFIX + STRETCH, HK, DH)
        value_rows = jnp.concatenate([old_values, new_values], axis=0).astype(jnp.float32).reshape(PREFIX + STRETCH, HK, DH)

        def one_block(offset):
            query_block = lax.dynamic_slice_in_dim(query_rows, offset, block, 0).astype(jnp.float32).reshape(block, HK, group, DH)
            scores = jnp.einsum('rhgd,khd->rhgk', query_block, key_rows) * factor
            row_index = offset + jnp.arange(block, dtype=jnp.int32)
            live = jnp.where(key_index[None, :] < PREFIX, key_index[None, :] < length, key_index[None, :] - PREFIX <= row_index[:, None])
            live = live[:, None, None, :]
            top_score = lax.optimization_barrier(jnp.max(jnp.where(live, scores, -1e+30), axis=-1, keepdims=True))
            weights = jnp.where(live, jnp.exp(scores - top_score), 0.0)
            weight_sum = lax.optimization_barrier(jnp.sum(weights, axis=-1))
            rounded = lax.optimization_barrier(weights.astype(jnp.bfloat16)).astype(jnp.float32)
            mixed = jnp.einsum('rhgk,khd->rhgd', rounded, value_rows) / weight_sum[..., None]
            return mixed.reshape(block, HQ * DH).astype(jnp.bfloat16)
        offsets = jnp.arange(STRETCH // block, dtype=jnp.int32) * block
        attention = lax.map(one_block, offsets).reshape(STRETCH, HQ * DH)
        old_live = jnp.arange(PREFIX // PAGE, dtype=jnp.int32) * PAGE < length
        new_live = jnp.ones((STRETCH // PAGE,), dtype=bool)
        return (attention, page_bounds(old_keys, old_live), page_bounds(new_keys, new_live))
    attention, prefix_bounds, stretch_bounds = lax.map(one_sequence, (queries, stretch_keys, stretch_values, cache_keys, cache_values, prefix_len))
    return (attention, prefix_bounds, stretch_bounds)
```

```python
import functools
import math

import jax
import jax.numpy as jnp
from jax import lax
from jax.experimental import pallas as pl
from jax.experimental.pallas import tpu as pltpu
from jax.sharding import PartitionSpec as P

MESH = pl.DeviceIdType.MESH
DH = 128
PAGE = 16
GROUP = 8
WIDTH = GROUP * DH
NZ = 8
NX = 2
OWNERS = NX * NZ
CHUNK = 256
DEAD = -1e30
FACTOR = math.log2(math.e) / math.sqrt(DH)


def offset_of(k):
    t = k // 2
    half = (t + 1) // 2
    return k % 2, half * (1 - 2 * ((t + 1) % 2))


def kernel(
    plen_ref, q_hbm, sk_hbm, sv_hbm, ck_hbm, cv_hbm,
    out_hbm, pb_ref, sb_ref,
    q_st, c_st, s_st, q_in, c_in, s_in, o_st, scores,
    load_sem, c_send, c_recv, s_send, s_recv, q_send, q_recv, o_send, o_recv,
    fc_send, fc_recv, fs_send, fs_recv, own_sem,
):
    grp = lax.axis_index("grp")
    seq = lax.axis_index("seq")
    x, z, core = seq // (2 * NZ), (seq // 2) % NZ, seq % 2
    rows = q_hbm.shape[1]
    pre_rows = ck_hbm.shape[1]

    def place(px, pz, pc):
        return (px % NX) * (2 * NZ) + ((pz + NZ) % NZ) * 2 + pc

    def target(k):
        dx, dz = offset_of(k)
        return (x + dx) % NX, (z + dz + NZ) % NZ

    def origin(k):
        dx, dz = offset_of(k)
        return (x + dx) % NX, (z - dz + NZ) % NZ

    loads = [
        pltpu.make_async_copy(ck_hbm, c_st.at[:, 0], load_sem.at[0]),
        pltpu.make_async_copy(cv_hbm, c_st.at[:, 1], load_sem.at[1]),
        pltpu.make_async_copy(sk_hbm, s_st.at[:, 0], load_sem.at[2]),
        pltpu.make_async_copy(sv_hbm, s_st.at[:, 1], load_sem.at[3]),
        pltpu.make_async_copy(q_hbm, q_st, load_sem.at[4]),
    ]
    for copy in loads:
        copy.start()

    barrier = pltpu.get_barrier_semaphore()
    for k in range(1, OWNERS):
        tx, tz = target(k)
        pl.semaphore_signal(
            barrier, inc=1, device_id=(grp, place(tx, tz, core)), device_id_type=MESH
        )
    partner = (grp, place(x, z, 1 - core))
    pl.semaphore_signal(barrier, inc=1, device_id=partner, device_id_type=MESH)
    for copy in loads:
        copy.wait()
    pl.semaphore_wait(barrier, OWNERS)

    def cols(g, width):
        return pl.ds(pl.multiple_of(g * width, width), width)

    def c_rows(i):
        return pl.ds(pl.multiple_of(i * pre_rows, pre_rows), pre_rows)

    def s_rows(i):
        return pl.ds(pl.multiple_of(i * rows, rows), rows)

    def c_copy(k):
        tx, tz = target(k)
        return pltpu.make_async_remote_copy(
            src_ref=c_st.at[tx, :, :, cols(tz, DH)], dst_ref=c_in.at[:, c_rows(seq)],
            send_sem=c_send.at[k], recv_sem=c_recv.at[k],
            device_id=(grp, place(tx, tz, core)), device_id_type=MESH,
        )

    def s_copy(k):
        tx, tz = target(k)
        return pltpu.make_async_remote_copy(
            src_ref=s_st.at[tx, :, :, cols(tz, DH)], dst_ref=s_in.at[:, s_rows(seq)],
            send_sem=s_send.at[k], recv_sem=s_recv.at[k],
            device_id=(grp, place(tx, tz, core)), device_id_type=MESH,
        )

    def q_copy(k):
        tx, tz = target(k)
        return pltpu.make_async_remote_copy(
            src_ref=q_st.at[tx, :, cols(tz, WIDTH)], dst_ref=q_in.at[k],
            send_sem=q_send.at[k], recv_sem=q_recv.at[k],
            device_id=(grp, place(tx, tz, core)), device_id_type=MESH,
        )

    def o_copy(k):
        ox, oz = origin(k)
        return pltpu.make_async_remote_copy(
            src_ref=o_st.at[k], dst_ref=out_hbm.at[x, :, cols(z, WIDTH)],
            send_sem=o_send.at[k], recv_sem=o_recv.at[k],
            device_id=(grp, place(ox, oz, core)), device_id_type=MESH,
        )

    def forward(k):
        ox, oz = origin(k)
        i = place(ox, oz, core)
        return (
            pltpu.make_async_remote_copy(
                src_ref=c_in.at[:, c_rows(i)], dst_ref=c_in.at[:, c_rows(i)],
                send_sem=fc_send.at[k], recv_sem=fc_recv.at[k],
                device_id=partner, device_id_type=MESH,
            ),
            pltpu.make_async_remote_copy(
                src_ref=s_in.at[:, s_rows(i)], dst_ref=s_in.at[:, s_rows(i)],
                send_sem=fs_send.at[k], recv_sem=fs_recv.at[k],
                device_id=partner, device_id_type=MESH,
            ),
        )

    for k in range(1, OWNERS):
        c_copy(k).start()
        s_copy(k).start()
    for k in range(1, OWNERS):
        q_copy(k).start()

    own = [
        pltpu.make_async_copy(c_st.at[x, :, :, cols(z, DH)], c_in.at[:, c_rows(seq)], own_sem.at[0]),
        pltpu.make_async_copy(s_st.at[x, :, :, cols(z, DH)], s_in.at[:, s_rows(seq)], own_sem.at[1]),
        pltpu.make_async_copy(q_st.at[x, :, cols(z, WIDTH)], q_in.at[0], own_sem.at[2]),
    ]
    for copy in own:
        copy.start()

    page0 = seq * (pre_rows // PAGE)

    def bounds(held, s, pages):
        lows, highs = [], []
        for p in range(pages):
            page = held[s, 0, p * PAGE:(p + 1) * PAGE, :].astype(jnp.float32)
            lows.append(jnp.min(page, axis=0, keepdims=True))
            highs.append(jnp.max(page, axis=0, keepdims=True))
        return jnp.concatenate(
            [jnp.concatenate(lows, axis=0), jnp.concatenate(highs, axis=0)], axis=1
        )

    for s in range(c_st.shape[0]):
        pages = pre_rows // PAGE
        both = bounds(c_st, s, pages)
        page = page0 + lax.broadcasted_iota(jnp.int32, both.shape, 0)
        pb_ref[s] = jnp.where(page * PAGE < plen_ref[s], both, 0.0).astype(jnp.bfloat16)
        sb_ref[s] = bounds(s_st, s, rows // PAGE).astype(jnp.bfloat16)

    for copy in own:
        copy.wait()
    for k in range(OWNERS):
        if k:
            c_copy(k).wait_recv()
            s_copy(k).wait_recv()
        for copy in forward(k):
            copy.start()
    for k in range(OWNERS):
        for copy in forward(k):
            copy.wait_recv()

    length = plen_ref[x]
    block_rows = GROUP * rows
    n_pre = c_in.shape[1] // CHUNK
    n_new = s_in.shape[1] // CHUNK

    def attend(k):
        ox, oz = origin(k)
        first = place(ox, oz, core) * rows
        q = jnp.concatenate([q_in[k, :, h * DH:(h + 1) * DH] for h in range(GROUP)], axis=0)
        lane = lax.broadcasted_iota(jnp.int32, (1, CHUNK), 1)
        row = first + lax.broadcasted_iota(jnp.int32, (block_rows, 1), 0) % rows
        top = jnp.full((block_rows, DH), DEAD, jnp.float32)
        for j in range(n_pre + n_new):
            if j < n_pre:
                key = c_in[0, j * CHUNK:(j + 1) * CHUNK, :]
                live = lane + j * CHUNK < length
            else:
                key = s_in[0, (j - n_pre) * CHUNK:(j - n_pre + 1) * CHUNK, :]
                live = lane + (j - n_pre) * CHUNK <= row
            s = lax.dot_general(
                q, key, (((1,), (1,)), ((), ())), preferred_element_type=jnp.float32
            )
            s = jnp.where(live, s, DEAD)
            scores[:, j * CHUNK:(j + 1) * CHUNK] = s
            for i in range(CHUNK // DH):
                top = jnp.maximum(top, s[:, i * DH:(i + 1) * DH])
        top = jnp.max(top, axis=1, keepdims=True)
        total = jnp.zeros((block_rows, DH), jnp.float32)
        acc = jnp.zeros((block_rows, DH), jnp.float32)
        for j in range(n_pre + n_new):
            if j < n_pre:
                value = c_in[1, j * CHUNK:(j + 1) * CHUNK, :]
            else:
                value = s_in[1, (j - n_pre) * CHUNK:(j - n_pre + 1) * CHUNK, :]
            w = jnp.exp2((scores[:, j * CHUNK:(j + 1) * CHUNK] - top) * FACTOR)
            for i in range(CHUNK // DH):
                total = total + w[:, i * DH:(i + 1) * DH]
            acc = acc + jnp.dot(
                w.astype(jnp.bfloat16), value, preferred_element_type=jnp.float32
            )
        out = (acc / jnp.sum(total, axis=1, keepdims=True)).astype(jnp.bfloat16)
        for h in range(GROUP):
            o_st[k, :, h * DH:(h + 1) * DH] = out[h * rows:(h + 1) * rows, :]

    def step(k, carry):
        q_copy(k).wait_recv()
        attend(k)

        @pl.when(k > 1)
        def _():
            o_copy(k - 1).start()

        return carry

    lax.fori_loop(1, OWNERS, step, 0)
    o_copy(OWNERS - 1).start()
    attend(0)
    mine = pltpu.make_async_copy(o_st.at[0], out_hbm.at[x, :, cols(z, WIDTH)], own_sem.at[0])
    mine.start()

    for k in range(1, OWNERS):
        c_copy(k).wait_send()
        s_copy(k).wait_send()
        q_copy(k).wait_send()
    for k in range(OWNERS):
        for copy in forward(k):
            copy.wait_send()
    for k in range(1, OWNERS):
        o_copy(k).wait()
    mine.wait()


def on_device(queries, stretch_keys, stretch_values, cache_keys, cache_values, prefix_len):
    seqs, rows, wide = queries.shape
    pre_rows, width = cache_keys.shape[1:]
    members = lax.axis_size("seq")
    dma = pltpu.SemaphoreType.DMA
    any_spec = pl.BlockSpec(memory_space=pl.ANY)
    vmem_spec = pl.BlockSpec(memory_space=pltpu.VMEM)
    attention, pb, sb = pl.pallas_call(
        kernel,
        out_shape=(
            jax.ShapeDtypeStruct((seqs, rows, wide), jnp.bfloat16),
            jax.ShapeDtypeStruct((seqs, pre_rows // PAGE, 2 * width), jnp.bfloat16),
            jax.ShapeDtypeStruct((seqs, rows // PAGE, 2 * width), jnp.bfloat16),
        ),
        in_specs=[pl.BlockSpec(memory_space=pltpu.SMEM)] + [any_spec] * 5,
        out_specs=(any_spec, vmem_spec, vmem_spec),
        scratch_shapes=[
            pltpu.VMEM((seqs, rows, wide), jnp.bfloat16),
            pltpu.VMEM((seqs, 2, pre_rows, width), jnp.bfloat16),
            pltpu.VMEM((seqs, 2, rows, width), jnp.bfloat16),
            pltpu.VMEM((OWNERS, rows, WIDTH), jnp.bfloat16),
            pltpu.VMEM((2, members * pre_rows, DH), jnp.bfloat16),
            pltpu.VMEM((2, members * rows, DH), jnp.bfloat16),
            pltpu.VMEM((OWNERS, rows, WIDTH), jnp.bfloat16),
            pltpu.VMEM((GROUP * rows, members * (pre_rows + rows)), jnp.float32),
            dma((5,)),
        ]
        + [dma((OWNERS,))] * 12
        + [dma((3,))],
        compiler_params=pltpu.CompilerParams(
            collective_id=0, has_side_effects=True, vmem_limit_bytes=56 * 2**20
        ),
        name="attend",
    )(prefix_len, queries, stretch_keys, stretch_values, cache_keys, cache_values)
    return attention, pb, sb


def solution(mesh):
    spec = P("grp", "seq", None)
    return jax.shard_map(
        on_device,
        mesh=mesh,
        in_specs=(spec, spec, spec, spec, spec, P("grp")),
        out_specs=(spec, spec, spec),
        check_vma=False,
    )
```

```python
import functools
import math

import jax
import jax.numpy as jnp
from jax import lax
from jax.experimental import pallas as pl
from jax.experimental.pallas import tpu as pltpu
from jax.sharding import PartitionSpec as P

MESH = pl.DeviceIdType.MESH
DH = 128
PAGE = 16
GROUP = 8
WIDTH = GROUP * DH
NZ = 8
NX = 2
OWNERS = NX * NZ
CHUNK = 256
DEAD = -1e30
FACTOR = math.log2(math.e) / math.sqrt(DH)


def offset_of(k):
    t = k // 2
    half = (t + 1) // 2
    return k % 2, half * (1 - 2 * ((t + 1) % 2))


def kernel(
    plen_ref, q_hbm, sk_hbm, sv_hbm, ck_hbm, cv_hbm,
    out_ref, pb_ref, sb_ref,
    q_st, c_st, s_st, q_in, c_in, s_in, o_st, scores,
    load_sem, c_send, c_recv, s_send, s_recv, q_send, q_recv, o_send, o_recv,
    fc_send, fc_recv, fs_send, fs_recv, own_sem, chain,
):
    grp = lax.axis_index("grp")
    seq = lax.axis_index("seq")
    x, z, core = seq // (2 * NZ), (seq // 2) % NZ, seq % 2
    rows = q_hbm.shape[1]
    pre_rows = ck_hbm.shape[1]

    def place(px, pz, pc):
        return (px % NX) * (2 * NZ) + ((pz + NZ) % NZ) * 2 + pc

    def target(k):
        dx, dz = offset_of(k)
        return (x + dx) % NX, (z + dz + NZ) % NZ

    def origin(k):
        dx, dz = offset_of(k)
        return (x + dx) % NX, (z - dz + NZ) % NZ

    loads = [
        pltpu.make_async_copy(ck_hbm, c_st.at[:, 0], load_sem.at[0]),
        pltpu.make_async_copy(cv_hbm, c_st.at[:, 1], load_sem.at[1]),
        pltpu.make_async_copy(sk_hbm, s_st.at[:, 0], load_sem.at[2]),
        pltpu.make_async_copy(sv_hbm, s_st.at[:, 1], load_sem.at[3]),
        pltpu.make_async_copy(q_hbm, q_st, load_sem.at[4]),
    ]
    for copy in loads:
        copy.start()

    partner = (grp, place(x, z, 1 - core))
    above, below = (grp, place(x, z + 1, core)), (grp, place(x, z - 1, core))
    across = (grp, place(x + 1, z, core))
    barrier = pltpu.get_barrier_semaphore()
    for near in (above, below, across, partner):
        pl.semaphore_signal(barrier, inc=1, device_id=near, device_id_type=MESH)

    def tell(level):
        pl.semaphore_signal(chain.at[0, level], inc=1, device_id=above, device_id_type=MESH)
        pl.semaphore_signal(chain.at[1, level], inc=1, device_id=below, device_id_type=MESH)

    def hear(level):
        pl.semaphore_wait(chain.at[0, level], 1)
        pl.semaphore_wait(chain.at[1, level], 1)

    def cols(g, width):
        return pl.ds(pl.multiple_of(g * width, width), width)

    def c_rows(i):
        return pl.ds(pl.multiple_of(i * pre_rows, pre_rows), pre_rows)

    def s_rows(i):
        return pl.ds(pl.multiple_of(i * rows, rows), rows)

    def c_copy(k):
        tx, tz = target(k)
        return pltpu.make_async_remote_copy(
            src_ref=c_st.at[tx, :, :, cols(tz, DH)], dst_ref=c_in.at[:, c_rows(seq)],
            send_sem=c_send.at[k], recv_sem=c_recv.at[k],
            device_id=(grp, place(tx, tz, core)), device_id_type=MESH,
        )

    def s_copy(k):
        tx, tz = target(k)
        return pltpu.make_async_remote_copy(
            src_ref=s_st.at[tx, :, :, cols(tz, DH)], dst_ref=s_in.at[:, s_rows(seq)],
            send_sem=s_send.at[k], recv_sem=s_recv.at[k],
            device_id=(grp, place(tx, tz, core)), device_id_type=MESH,
        )

    def q_copy(k):
        tx, tz = target(k)
        return pltpu.make_async_remote_copy(
            src_ref=q_st.at[tx, :, cols(tz, WIDTH)], dst_ref=q_in.at[k],
            send_sem=q_send.at[k], recv_sem=q_recv.at[k],
            device_id=(grp, place(tx, tz, core)), device_id_type=MESH,
        )

    def o_copy(k):
        ox, oz = origin(k)
        return pltpu.make_async_remote_copy(
            src_ref=o_st.at[k], dst_ref=out_ref.at[x, :, cols(z, WIDTH)],
            send_sem=o_send.at[k], recv_sem=o_recv.at[k],
            device_id=(grp, place(ox, oz, core)), device_id_type=MESH,
        )

    def forward(k):
        ox, oz = origin(k)
        i = place(ox, oz, core)
        return (
            pltpu.make_async_remote_copy(
                src_ref=c_in.at[:, c_rows(i)], dst_ref=c_in.at[:, c_rows(i)],
                send_sem=fc_send.at[k], recv_sem=fc_recv.at[k],
                device_id=partner, device_id_type=MESH,
            ),
            pltpu.make_async_remote_copy(
                src_ref=s_in.at[:, s_rows(i)], dst_ref=s_in.at[:, s_rows(i)],
                send_sem=fs_send.at[k], recv_sem=fs_recv.at[k],
                device_id=partner, device_id_type=MESH,
            ),
        )

    def give(*partners):
        for k in partners:
            c_copy(k).start()
            s_copy(k).start()

    for copy in loads[:4]:
        copy.wait()
    pl.semaphore_wait(barrier, 4)
    tell(0)
    give(2, 4, 1)
    hear(0)
    tell(1)
    give(3, 5, 6, 8)
    hear(1)
    tell(2)
    give(7, 9, 10, 12)
    hear(2)
    tell(3)
    give(11, 13, 14)
    hear(3)
    give(15)
    loads[4].wait()
    for k in range(1, OWNERS):
        q_copy(k).start()

    own = [
        pltpu.make_async_copy(c_st.at[x, :, :, cols(z, DH)], c_in.at[:, c_rows(seq)], own_sem.at[0]),
        pltpu.make_async_copy(s_st.at[x, :, :, cols(z, DH)], s_in.at[:, s_rows(seq)], own_sem.at[1]),
        pltpu.make_async_copy(q_st.at[x, :, cols(z, WIDTH)], q_in.at[0], own_sem.at[2]),
    ]
    for copy in own:
        copy.start()

    page0 = seq * (pre_rows // PAGE)

    def bounds(held, s, pages):
        lows, highs = [], []
        for p in range(pages):
            page = held[s, 0, p * PAGE:(p + 1) * PAGE, :].astype(jnp.float32)
            lows.append(jnp.min(page, axis=0, keepdims=True))
            highs.append(jnp.max(page, axis=0, keepdims=True))
        return jnp.concatenate(
            [jnp.concatenate(lows, axis=0), jnp.concatenate(highs, axis=0)], axis=1
        )

    for s in range(c_st.shape[0]):
        pages = pre_rows // PAGE
        both = bounds(c_st, s, pages)
        page = page0 + lax.broadcasted_iota(jnp.int32, both.shape, 0)
        pb_ref[s] = jnp.where(page * PAGE < plen_ref[s], both, 0.0).astype(jnp.bfloat16)
        sb_ref[s] = bounds(s_st, s, rows // PAGE).astype(jnp.bfloat16)

    for copy in own:
        copy.wait()
    for k in range(OWNERS):
        if k:
            c_copy(k).wait_recv()
            s_copy(k).wait_recv()
        for copy in forward(k):
            copy.start()
    for k in range(OWNERS):
        for copy in forward(k):
            copy.wait_recv()

    length = plen_ref[x]
    block_rows = GROUP * rows
    n_pre = c_in.shape[1] // CHUNK
    n_new = s_in.shape[1] // CHUNK

    def attend(k):
        ox, oz = origin(k)
        first = place(ox, oz, core) * rows
        q = jnp.concatenate([q_in[k, :, h * DH:(h + 1) * DH] for h in range(GROUP)], axis=0)
        lane = lax.broadcasted_iota(jnp.int32, (1, CHUNK), 1)
        row = first + lax.broadcasted_iota(jnp.int32, (block_rows, 1), 0) % rows
        top = jnp.full((block_rows, DH), DEAD, jnp.float32)
        for j in range(n_pre + n_new):
            if j < n_pre:
                key = c_in[0, j * CHUNK:(j + 1) * CHUNK, :]
                live = lane + j * CHUNK < length
            else:
                key = s_in[0, (j - n_pre) * CHUNK:(j - n_pre + 1) * CHUNK, :]
                live = lane + (j - n_pre) * CHUNK <= row
            s = lax.dot_general(
                q, key, (((1,), (1,)), ((), ())), preferred_element_type=jnp.float32
            )
            s = jnp.where(live, s, DEAD)
            scores[:, j * CHUNK:(j + 1) * CHUNK] = s
            for i in range(CHUNK // DH):
                top = jnp.maximum(top, s[:, i * DH:(i + 1) * DH])
        top = jnp.max(top, axis=1, keepdims=True)
        total = jnp.zeros((block_rows, DH), jnp.float32)
        acc = jnp.zeros((block_rows, DH), jnp.float32)
        for j in range(n_pre + n_new):
            if j < n_pre:
                value = c_in[1, j * CHUNK:(j + 1) * CHUNK, :]
            else:
                value = s_in[1, (j - n_pre) * CHUNK:(j - n_pre + 1) * CHUNK, :]
            w = jnp.exp2((scores[:, j * CHUNK:(j + 1) * CHUNK] - top) * FACTOR)
            for i in range(CHUNK // DH):
                total = total + w[:, i * DH:(i + 1) * DH]
            acc = acc + jnp.dot(
                w.astype(jnp.bfloat16), value, preferred_element_type=jnp.float32
            )
        out = (acc / jnp.sum(total, axis=1, keepdims=True)).astype(jnp.bfloat16)
        for h in range(GROUP):
            o_st[k, :, h * DH:(h + 1) * DH] = out[h * rows:(h + 1) * rows, :]

    def step(k, carry):
        q_copy(k).wait_recv()
        attend(k)

        @pl.when(k > 1)
        def _():
            o_copy(k - 1).start()

        return carry

    lax.fori_loop(1, OWNERS, step, 0)
    o_copy(OWNERS - 1).start()
    attend(0)
    mine = pltpu.make_async_copy(o_st.at[0], out_ref.at[x, :, cols(z, WIDTH)], own_sem.at[0])
    mine.start()

    for k in range(1, OWNERS):
        c_copy(k).wait_send()
        s_copy(k).wait_send()
        q_copy(k).wait_send()
    for k in range(OWNERS):
        for copy in forward(k):
            copy.wait_send()
    for k in range(1, OWNERS):
        o_copy(k).wait()
    mine.wait()


def on_device(queries, stretch_keys, stretch_values, cache_keys, cache_values, prefix_len):
    seqs, rows, wide = queries.shape
    pre_rows, width = cache_keys.shape[1:]
    members = lax.axis_size("seq")
    dma = pltpu.SemaphoreType.DMA
    any_spec = pl.BlockSpec(memory_space=pl.ANY)
    vmem_spec = pl.BlockSpec(memory_space=pltpu.VMEM)
    shapes = (
        (seqs, rows, wide),
        (seqs, pre_rows // PAGE, 2 * width),
        (seqs, rows // PAGE, 2 * width),
    )
    return pl.pallas_call(
        kernel,
        out_shape=tuple(pltpu.VMEM(shape, jnp.bfloat16) for shape in shapes),
        in_specs=[pl.BlockSpec(memory_space=pltpu.SMEM)] + [any_spec] * 5,
        out_specs=(vmem_spec,) * 3,
        scratch_shapes=[
            pltpu.VMEM((seqs, rows, wide), jnp.bfloat16),
            pltpu.VMEM((seqs, 2, pre_rows, width), jnp.bfloat16),
            pltpu.VMEM((seqs, 2, rows, width), jnp.bfloat16),
            pltpu.VMEM((OWNERS, rows, WIDTH), jnp.bfloat16),
            pltpu.VMEM((2, members * pre_rows, DH), jnp.bfloat16),
            pltpu.VMEM((2, members * rows, DH), jnp.bfloat16),
            pltpu.VMEM((OWNERS, rows, WIDTH), jnp.bfloat16),
            pltpu.VMEM((GROUP * rows, members * (pre_rows + rows)), jnp.float32),
            dma((5,)),
        ]
        + [dma((OWNERS,))] * 12
        + [dma((3,)), pltpu.SemaphoreType.REGULAR((2, NZ // 2))],
        compiler_params=pltpu.CompilerParams(
            collective_id=0, has_side_effects=True, vmem_limit_bytes=56 * 2**20
        ),
        name="attend",
    )(prefix_len, queries, stretch_keys, stretch_values, cache_keys, cache_values)

def solution(mesh):
    spec = P("grp", "seq", None)
    return jax.shard_map(
        on_device,
        mesh=mesh,
        in_specs=(spec, spec, spec, spec, spec, P("grp")),
        out_specs=(spec, spec, spec),
        check_vma=False,
    )
```

```python
import functools
import math

import jax
import jax.numpy as jnp
from jax import lax
from jax.experimental import pallas as pl
from jax.experimental.pallas import tpu as pltpu
from jax.sharding import PartitionSpec as P

MESH = pl.DeviceIdType.MESH
DH = 128
PAGE = 16
GROUP = 8
WIDTH = GROUP * DH
NZ = 8
NX = 2
OWNERS = NX * NZ
CHUNK = 256
DEAD = -1e30
FACTOR = math.log2(math.e) / math.sqrt(DH)


def offset_of(k):
    t = k // 2
    half = (t + 1) // 2
    return k % 2, half * (1 - 2 * ((t + 1) % 2))


def kernel(
    plen_ref, q_hbm, sk_hbm, sv_hbm, ck_hbm, cv_hbm,
    out_ref, pb_ref, sb_ref,
    q_st, c_st, s_st, q_in, c_in, s_in, o_st, scores,
    load_sem, c_send, c_recv, s_send, s_recv, q_send, q_recv, o_send, o_recv,
    fc_send, fc_recv, fs_send, fs_recv, own_sem, chain,
):
    grp = lax.axis_index("grp")
    seq = lax.axis_index("seq")
    x, z, core = seq // (2 * NZ), (seq // 2) % NZ, seq % 2
    rows = q_hbm.shape[1]
    pre_rows = ck_hbm.shape[1]

    def place(px, pz, pc):
        return (px % NX) * (2 * NZ) + ((pz + NZ) % NZ) * 2 + pc

    def target(k):
        dx, dz = offset_of(k)
        return (x + dx) % NX, (z + dz + NZ) % NZ

    def origin(k):
        dx, dz = offset_of(k)
        return (x + dx) % NX, (z - dz + NZ) % NZ

    loads = [
        pltpu.make_async_copy(ck_hbm, c_st.at[:, 0], load_sem.at[0]),
        pltpu.make_async_copy(cv_hbm, c_st.at[:, 1], load_sem.at[1]),
        pltpu.make_async_copy(sk_hbm, s_st.at[:, 0], load_sem.at[2]),
        pltpu.make_async_copy(sv_hbm, s_st.at[:, 1], load_sem.at[3]),
        pltpu.make_async_copy(q_hbm, q_st, load_sem.at[4]),
    ]
    for copy in loads:
        copy.start()

    partner = (grp, place(x, z, 1 - core))
    above, below = (grp, place(x, z + 1, core)), (grp, place(x, z - 1, core))
    across = (grp, place(x + 1, z, core))
    barrier = pltpu.get_barrier_semaphore()
    for near in (above, below, across, partner):
        pl.semaphore_signal(barrier, inc=1, device_id=near, device_id_type=MESH)

    def tell(level):
        pl.semaphore_signal(chain.at[0, level], inc=1, device_id=above, device_id_type=MESH)
        pl.semaphore_signal(chain.at[1, level], inc=1, device_id=below, device_id_type=MESH)

    def hear(level):
        pl.semaphore_wait(chain.at[0, level], 1)
        pl.semaphore_wait(chain.at[1, level], 1)

    def cols(g, width):
        return pl.ds(pl.multiple_of(g * width, width), width)

    def c_rows(i):
        return pl.ds(pl.multiple_of(i * pre_rows, pre_rows), pre_rows)

    def s_rows(i):
        return pl.ds(pl.multiple_of(i * rows, rows), rows)

    def c_copy(k):
        tx, tz = target(k)
        return pltpu.make_async_remote_copy(
            src_ref=c_st.at[tx, :, :, cols(tz, DH)], dst_ref=c_in.at[:, c_rows(seq)],
            send_sem=c_send.at[k], recv_sem=c_recv.at[k],
            device_id=(grp, place(tx, tz, core)), device_id_type=MESH,
        )

    def s_copy(k):
        tx, tz = target(k)
        return pltpu.make_async_remote_copy(
            src_ref=s_st.at[tx, :, :, cols(tz, DH)], dst_ref=s_in.at[:, s_rows(seq)],
            send_sem=s_send.at[k], recv_sem=s_recv.at[k],
            device_id=(grp, place(tx, tz, core)), device_id_type=MESH,
        )

    def q_copy(k):
        tx, tz = target(k)
        return pltpu.make_async_remote_copy(
            src_ref=q_st.at[tx, :, cols(tz, WIDTH)], dst_ref=q_in.at[k],
            send_sem=q_send.at[k], recv_sem=q_recv.at[k],
            device_id=(grp, place(tx, tz, core)), device_id_type=MESH,
        )

    def o_copy(k):
        ox, oz = origin(k)
        return pltpu.make_async_remote_copy(
            src_ref=o_st.at[k], dst_ref=out_ref.at[x, :, cols(z, WIDTH)],
            send_sem=o_send.at[k], recv_sem=o_recv.at[k],
            device_id=(grp, place(ox, oz, core)), device_id_type=MESH,
        )

    def forward(k):
        ox, oz = origin(k)
        i = place(ox, oz, core)
        return (
            pltpu.make_async_remote_copy(
                src_ref=c_in.at[:, c_rows(i)], dst_ref=c_in.at[:, c_rows(i)],
                send_sem=fc_send.at[k], recv_sem=fc_recv.at[k],
                device_id=partner, device_id_type=MESH,
            ),
            pltpu.make_async_remote_copy(
                src_ref=s_in.at[:, s_rows(i)], dst_ref=s_in.at[:, s_rows(i)],
                send_sem=fs_send.at[k], recv_sem=fs_recv.at[k],
                device_id=partner, device_id_type=MESH,
            ),
        )

    def give(*partners):
        for k in partners:
            c_copy(k).start()
            s_copy(k).start()

    for copy in loads[:4]:
        copy.wait()
    pl.semaphore_wait(barrier, 4)
    tell(0)
    give(2, 4, 1)
    hear(0)
    tell(1)
    give(3, 5, 6, 8)
    hear(1)
    tell(2)
    give(7, 9, 10, 12)
    hear(2)
    tell(3)
    give(11, 13, 14)
    hear(3)
    give(15)
    loads[4].wait()
    for k in reversed(range(1, OWNERS)):
        q_copy(k).start()

    own = [
        pltpu.make_async_copy(c_st.at[x, :, :, cols(z, DH)], c_in.at[:, c_rows(seq)], own_sem.at[0]),
        pltpu.make_async_copy(s_st.at[x, :, :, cols(z, DH)], s_in.at[:, s_rows(seq)], own_sem.at[1]),
        pltpu.make_async_copy(q_st.at[x, :, cols(z, WIDTH)], q_in.at[0], own_sem.at[2]),
    ]
    for copy in own:
        copy.start()

    page0 = seq * (pre_rows // PAGE)

    def bounds(held, s, pages):
        lows, highs = [], []
        for p in range(pages):
            page = held[s, 0, p * PAGE:(p + 1) * PAGE, :].astype(jnp.float32)
            lows.append(jnp.min(page, axis=0, keepdims=True))
            highs.append(jnp.max(page, axis=0, keepdims=True))
        return jnp.concatenate(
            [jnp.concatenate(lows, axis=0), jnp.concatenate(highs, axis=0)], axis=1
        )

    for s in range(c_st.shape[0]):
        pages = pre_rows // PAGE
        both = bounds(c_st, s, pages)
        page = page0 + lax.broadcasted_iota(jnp.int32, both.shape, 0)
        pb_ref[s] = jnp.where(page * PAGE < plen_ref[s], both, 0.0).astype(jnp.bfloat16)
        sb_ref[s] = bounds(s_st, s, rows // PAGE).astype(jnp.bfloat16)

    for copy in own:
        copy.wait()
    for k in range(OWNERS):
        if k:
            c_copy(k).wait_recv()
            s_copy(k).wait_recv()
        for copy in forward(k):
            copy.start()
    for k in range(OWNERS):
        for copy in forward(k):
            copy.wait_recv()

    length = plen_ref[x]
    block_rows = GROUP * rows
    n_pre = c_in.shape[1] // CHUNK
    n_new = s_in.shape[1] // CHUNK

    def attend(k):
        ox, oz = origin(k)
        first = place(ox, oz, core) * rows
        q = jnp.concatenate([q_in[k, :, h * DH:(h + 1) * DH] for h in range(GROUP)], axis=0)
        lane = lax.broadcasted_iota(jnp.int32, (1, CHUNK), 1)
        row = first + lax.broadcasted_iota(jnp.int32, (block_rows, 1), 0) % rows
        top = jnp.full((block_rows, DH), DEAD, jnp.float32)
        for j in range(n_pre + n_new):
            if j < n_pre:
                key = c_in[0, j * CHUNK:(j + 1) * CHUNK, :]
                live = lane + j * CHUNK < length
            else:
                key = s_in[0, (j - n_pre) * CHUNK:(j - n_pre + 1) * CHUNK, :]
                live = lane + (j - n_pre) * CHUNK <= row
            s = lax.dot_general(
                q, key, (((1,), (1,)), ((), ())), preferred_element_type=jnp.float32
            )
            s = jnp.where(live, s, DEAD)
            scores[:, j * CHUNK:(j + 1) * CHUNK] = s
            for i in range(CHUNK // DH):
                top = jnp.maximum(top, s[:, i * DH:(i + 1) * DH])
        top = jnp.max(top, axis=1, keepdims=True)
        total = jnp.zeros((block_rows, DH), jnp.float32)
        acc = jnp.zeros((block_rows, DH), jnp.float32)
        for j in range(n_pre + n_new):
            if j < n_pre:
                value = c_in[1, j * CHUNK:(j + 1) * CHUNK, :]
            else:
                value = s_in[1, (j - n_pre) * CHUNK:(j - n_pre + 1) * CHUNK, :]
            w = jnp.exp2((scores[:, j * CHUNK:(j + 1) * CHUNK] - top) * FACTOR)
            for i in range(CHUNK // DH):
                total = total + w[:, i * DH:(i + 1) * DH]
            acc = acc + jnp.dot(
                w.astype(jnp.bfloat16), value, preferred_element_type=jnp.float32
            )
        out = (acc / jnp.sum(total, axis=1, keepdims=True)).astype(jnp.bfloat16)
        for h in range(GROUP):
            o_st[k, :, h * DH:(h + 1) * DH] = out[h * rows:(h + 1) * rows, :]

    def step(i, carry):
        k = OWNERS - 1 - i
        q_copy(k).wait_recv()
        attend(k)

        @pl.when(i > 0)
        def _():
            o_copy(k + 1).start()

        return carry

    lax.fori_loop(0, OWNERS - 1, step, 0)
    o_copy(1).start()
    attend(0)
    mine = pltpu.make_async_copy(o_st.at[0], out_ref.at[x, :, cols(z, WIDTH)], own_sem.at[0])
    mine.start()

    for k in range(1, OWNERS):
        c_copy(k).wait_send()
        s_copy(k).wait_send()
        q_copy(k).wait_send()
    for k in range(OWNERS):
        for copy in forward(k):
            copy.wait_send()
    for k in range(1, OWNERS):
        o_copy(k).wait()
    mine.wait()


def put_out(*refs):
    *ends, sem = refs
    half = len(ends) // 2
    copies = [pltpu.make_async_copy(ends[i], ends[half + i], sem.at[i]) for i in range(half)]
    for copy in copies:
        copy.start()
    for copy in copies:
        copy.wait()


def on_device(queries, stretch_keys, stretch_values, cache_keys, cache_values, prefix_len):
    seqs, rows, wide = queries.shape
    pre_rows, width = cache_keys.shape[1:]
    members = lax.axis_size("seq")
    dma = pltpu.SemaphoreType.DMA
    any_spec = pl.BlockSpec(memory_space=pl.ANY)
    vmem_spec = pl.BlockSpec(memory_space=pltpu.VMEM)
    shapes = (
        (seqs, rows, wide),
        (seqs, pre_rows // PAGE, 2 * width),
        (seqs, rows // PAGE, 2 * width),
    )
    held = pl.pallas_call(
        kernel,
        out_shape=tuple(pltpu.VMEM(shape, jnp.bfloat16) for shape in shapes),
        in_specs=[pl.BlockSpec(memory_space=pltpu.SMEM)] + [any_spec] * 5,
        out_specs=(vmem_spec,) * 3,
        scratch_shapes=[
            pltpu.VMEM((seqs, rows, wide), jnp.bfloat16),
            pltpu.VMEM((seqs, 2, pre_rows, width), jnp.bfloat16),
            pltpu.VMEM((seqs, 2, rows, width), jnp.bfloat16),
            pltpu.VMEM((OWNERS, rows, WIDTH), jnp.bfloat16),
            pltpu.VMEM((2, members * pre_rows, DH), jnp.bfloat16),
            pltpu.VMEM((2, members * rows, DH), jnp.bfloat16),
            pltpu.VMEM((OWNERS, rows, WIDTH), jnp.bfloat16),
            pltpu.VMEM((GROUP * rows, members * (pre_rows + rows)), jnp.float32),
            dma((5,)),
        ]
        + [dma((OWNERS,))] * 12
        + [dma((3,)), pltpu.SemaphoreType.REGULAR((2, NZ // 2))],
        compiler_params=pltpu.CompilerParams(
            collective_id=0, has_side_effects=True, vmem_limit_bytes=56 * 2**20
        ),
        name="attend",
    )(prefix_len, queries, stretch_keys, stretch_values, cache_keys, cache_values)
    held = [pltpu.with_memory_space_constraint(array, pltpu.VMEM) for array in held]
    return pl.pallas_call(
        put_out,
        out_shape=tuple(jax.ShapeDtypeStruct(shape, jnp.bfloat16) for shape in shapes),
        in_specs=[vmem_spec] * 3,
        out_specs=(any_spec,) * 3,
        scratch_shapes=[dma((3,))],
        name="put_out",
    )(*held)

def solution(mesh):
    spec = P("grp", "seq", None)
    return jax.shard_map(
        on_device,
        mesh=mesh,
        in_specs=(spec, spec, spec, spec, spec, P("grp")),
        out_specs=(spec, spec, spec),
        check_vma=False,
    )
```

```python
import functools
import math

import jax
import jax.numpy as jnp
from jax import lax
from jax.experimental import pallas as pl
from jax.experimental.pallas import tpu as pltpu
from jax.sharding import PartitionSpec as P

MESH = pl.DeviceIdType.MESH
DH = 128
PAGE = 16
GROUP = 8
WIDTH = GROUP * DH
NZ = 8
NX = 2
OWNERS = NX * NZ
CHUNK = 256
DEAD = -1e30
FACTOR = math.log2(math.e) / math.sqrt(DH)


def offset_of(k):
    t = k // 2
    half = (t + 1) // 2
    return k % 2, half * (1 - 2 * ((t + 1) % 2))


def kernel(
    plen_ref, q_hbm, sk_hbm, sv_hbm, ck_hbm, cv_hbm,
    out_ref, pb_ref, sb_ref,
    q_st, c_st, s_st, q_in, c_in, s_in, o_st, scores,
    load_sem, c_send, c_recv, s_send, s_recv, q_send, q_recv, o_send, o_recv,
    fc_send, fc_recv, fs_send, fs_recv, own_sem, chain,
):
    grp = lax.axis_index("grp")
    seq = lax.axis_index("seq")
    x, z, core = seq // (2 * NZ), (seq // 2) % NZ, seq % 2
    rows = q_hbm.shape[1]
    pre_rows = ck_hbm.shape[1]

    def place(px, pz, pc):
        return (px % NX) * (2 * NZ) + ((pz + NZ) % NZ) * 2 + pc

    def target(k):
        dx, dz = offset_of(k)
        return (x + dx) % NX, (z + dz + NZ) % NZ

    def origin(k):
        dx, dz = offset_of(k)
        return (x + dx) % NX, (z - dz + NZ) % NZ

    loads = [
        pltpu.make_async_copy(ck_hbm, c_st.at[:, 0], load_sem.at[0]),
        pltpu.make_async_copy(cv_hbm, c_st.at[:, 1], load_sem.at[1]),
        pltpu.make_async_copy(sk_hbm, s_st.at[:, 0], load_sem.at[2]),
        pltpu.make_async_copy(sv_hbm, s_st.at[:, 1], load_sem.at[3]),
        pltpu.make_async_copy(q_hbm, q_st, load_sem.at[4]),
    ]

    partner = (grp, place(x, z, 1 - core))
    above, below = (grp, place(x, z + 1, core)), (grp, place(x, z - 1, core))
    across = (grp, place(x + 1, z, core))
    barrier = pltpu.get_barrier_semaphore()
    for near in (above, below, across, partner):
        pl.semaphore_signal(barrier, inc=1, device_id=near, device_id_type=MESH)

    for copy in loads:
        copy.start()

    def tell(level):
        pl.semaphore_signal(chain.at[0, level], inc=1, device_id=above, device_id_type=MESH)
        pl.semaphore_signal(chain.at[1, level], inc=1, device_id=below, device_id_type=MESH)

    def hear(level):
        pl.semaphore_wait(chain.at[0, level], 1)
        pl.semaphore_wait(chain.at[1, level], 1)

    def cols(g, width):
        return pl.ds(pl.multiple_of(g * width, width), width)

    def c_rows(i):
        return pl.ds(pl.multiple_of(i * pre_rows, pre_rows), pre_rows)

    def s_rows(i):
        return pl.ds(pl.multiple_of(i * rows, rows), rows)

    def c_copy(k):
        tx, tz = target(k)
        return pltpu.make_async_remote_copy(
            src_ref=c_st.at[tx, :, :, cols(tz, DH)], dst_ref=c_in.at[:, c_rows(seq)],
            send_sem=c_send.at[k], recv_sem=c_recv.at[k],
            device_id=(grp, place(tx, tz, core)), device_id_type=MESH,
        )

    def s_copy(k):
        tx, tz = target(k)
        return pltpu.make_async_remote_copy(
            src_ref=s_st.at[tx, :, :, cols(tz, DH)], dst_ref=s_in.at[:, s_rows(seq)],
            send_sem=s_send.at[k], recv_sem=s_recv.at[k],
            device_id=(grp, place(tx, tz, core)), device_id_type=MESH,
        )

    def q_copy(k):
        tx, tz = target(k)
        return pltpu.make_async_remote_copy(
            src_ref=q_st.at[tx, :, cols(tz, WIDTH)], dst_ref=q_in.at[k],
            send_sem=q_send.at[k], recv_sem=q_recv.at[k],
            device_id=(grp, place(tx, tz, core)), device_id_type=MESH,
        )

    def o_copy(k):
        ox, oz = origin(k)
        return pltpu.make_async_remote_copy(
            src_ref=o_st.at[k], dst_ref=out_ref.at[x, :, cols(z, WIDTH)],
            send_sem=o_send.at[k], recv_sem=o_recv.at[k],
            device_id=(grp, place(ox, oz, core)), device_id_type=MESH,
        )

    def forward(k):
        ox, oz = origin(k)
        i = place(ox, oz, core)
        return (
            pltpu.make_async_remote_copy(
                src_ref=c_in.at[:, c_rows(i)], dst_ref=c_in.at[:, c_rows(i)],
                send_sem=fc_send.at[k], recv_sem=fc_recv.at[k],
                device_id=partner, device_id_type=MESH,
            ),
            pltpu.make_async_remote_copy(
                src_ref=s_in.at[:, s_rows(i)], dst_ref=s_in.at[:, s_rows(i)],
                send_sem=fs_send.at[k], recv_sem=fs_recv.at[k],
                device_id=partner, device_id_type=MESH,
            ),
        )

    def give(*partners):
        for k in partners:
            c_copy(k).start()
            s_copy(k).start()

    for copy in loads[:4]:
        copy.wait()
    pl.semaphore_wait(barrier, 4)
    tell(0)
    give(2, 4)
    hear(0)
    tell(1)
    give(6, 8, 3, 5)
    hear(1)
    tell(2)
    give(10, 12, 7, 9)
    hear(2)
    tell(3)
    give(14, 11, 13)
    hear(3)
    give(15, 1)
    loads[4].wait()
    for k in reversed(range(1, OWNERS)):
        q_copy(k).start()

    own = [
        pltpu.make_async_copy(c_st.at[x, :, :, cols(z, DH)], c_in.at[:, c_rows(seq)], own_sem.at[0]),
        pltpu.make_async_copy(s_st.at[x, :, :, cols(z, DH)], s_in.at[:, s_rows(seq)], own_sem.at[1]),
        pltpu.make_async_copy(q_st.at[x, :, cols(z, WIDTH)], q_in.at[0], own_sem.at[2]),
    ]
    for copy in own:
        copy.start()

    page0 = seq * (pre_rows // PAGE)

    def bounds(held, s, pages):
        lows, highs = [], []
        for p in range(pages):
            page = held[s, 0, p * PAGE:(p + 1) * PAGE, :].astype(jnp.float32)
            lows.append(jnp.min(page, axis=0, keepdims=True))
            highs.append(jnp.max(page, axis=0, keepdims=True))
        return jnp.concatenate(
            [jnp.concatenate(lows, axis=0), jnp.concatenate(highs, axis=0)], axis=1
        )

    for s in range(c_st.shape[0]):
        pages = pre_rows // PAGE
        both = bounds(c_st, s, pages)
        page = page0 + lax.broadcasted_iota(jnp.int32, both.shape, 0)
        pb_ref[s] = jnp.where(page * PAGE < plen_ref[s], both, 0.0).astype(jnp.bfloat16)
        sb_ref[s] = bounds(s_st, s, rows // PAGE).astype(jnp.bfloat16)

    for copy in own:
        copy.wait()
    for k in range(OWNERS):
        if k:
            c_copy(k).wait_recv()
            s_copy(k).wait_recv()
        for copy in forward(k):
            copy.start()
    for k in range(OWNERS):
        for copy in forward(k):
            copy.wait_recv()

    length = plen_ref[x]
    block_rows = GROUP * rows
    n_pre = c_in.shape[1] // CHUNK
    n_new = s_in.shape[1] // CHUNK

    def attend(k):
        ox, oz = origin(k)
        first = place(ox, oz, core) * rows
        q = jnp.concatenate([q_in[k, :, h * DH:(h + 1) * DH] for h in range(GROUP)], axis=0)
        lane = lax.broadcasted_iota(jnp.int32, (1, CHUNK), 1)
        row = first + lax.broadcasted_iota(jnp.int32, (block_rows, 1), 0) % rows
        top = jnp.full((block_rows, DH), DEAD, jnp.float32)
        for j in range(n_pre + n_new):
            if j < n_pre:
                key = c_in[0, j * CHUNK:(j + 1) * CHUNK, :]
                live = lane + j * CHUNK < length
            else:
                key = s_in[0, (j - n_pre) * CHUNK:(j - n_pre + 1) * CHUNK, :]
                live = lane + (j - n_pre) * CHUNK <= row
            s = lax.dot_general(
                q, key, (((1,), (1,)), ((), ())), preferred_element_type=jnp.float32
            )
            s = jnp.where(live, s, DEAD)
            scores[:, j * CHUNK:(j + 1) * CHUNK] = s
            for i in range(CHUNK // DH):
                top = jnp.maximum(top, s[:, i * DH:(i + 1) * DH])
        top = jnp.max(top, axis=1, keepdims=True)
        total = jnp.zeros((block_rows, DH), jnp.float32)
        acc = jnp.zeros((block_rows, DH), jnp.float32)
        for j in range(n_pre + n_new):
            if j < n_pre:
                value = c_in[1, j * CHUNK:(j + 1) * CHUNK, :]
            else:
                value = s_in[1, (j - n_pre) * CHUNK:(j - n_pre + 1) * CHUNK, :]
            w = jnp.exp2((scores[:, j * CHUNK:(j + 1) * CHUNK] - top) * FACTOR)
            for i in range(CHUNK // DH):
                total = total + w[:, i * DH:(i + 1) * DH]
            acc = acc + jnp.dot(
                w.astype(jnp.bfloat16), value, preferred_element_type=jnp.float32
            )
        out = (acc / jnp.sum(total, axis=1, keepdims=True)).astype(jnp.bfloat16)
        for h in range(GROUP):
            o_st[k, :, h * DH:(h + 1) * DH] = out[h * rows:(h + 1) * rows, :]

    def step(i, carry):
        k = OWNERS - 1 - i
        q_copy(k).wait_recv()
        attend(k)

        @pl.when(i > 0)
        def _():
            o_copy(k + 1).start()

        return carry

    lax.fori_loop(0, OWNERS - 1, step, 0)
    attend(0)
    o_copy(1).start()
    mine = pltpu.make_async_copy(o_st.at[0], out_ref.at[x, :, cols(z, WIDTH)], own_sem.at[0])

    for k in range(1, OWNERS):
        c_copy(k).wait_send()
        s_copy(k).wait_send()
        q_copy(k).wait_send()
    for k in range(OWNERS):
        for copy in forward(k):
            copy.wait_send()
    mine.start()
    for k in range(1, OWNERS):
        o_copy(k).wait()
    mine.wait()


def put_out(*refs):
    *ends, sem = refs
    half = len(ends) // 2
    copies = [pltpu.make_async_copy(ends[i], ends[half + i], sem.at[i]) for i in range(half)]
    for copy in copies:
        copy.start()
    for copy in copies:
        copy.wait()


def on_device(queries, stretch_keys, stretch_values, cache_keys, cache_values, prefix_len):
    seqs, rows, wide = queries.shape
    pre_rows, width = cache_keys.shape[1:]
    members = lax.axis_size("seq")
    dma = pltpu.SemaphoreType.DMA
    any_spec = pl.BlockSpec(memory_space=pl.ANY)
    vmem_spec = pl.BlockSpec(memory_space=pltpu.VMEM)
    shapes = (
        (seqs, rows, wide),
        (seqs, pre_rows // PAGE, 2 * width),
        (seqs, rows // PAGE, 2 * width),
    )
    held = pl.pallas_call(
        kernel,
        out_shape=tuple(pltpu.VMEM(shape, jnp.bfloat16) for shape in shapes),
        in_specs=[pl.BlockSpec(memory_space=pltpu.SMEM)] + [any_spec] * 5,
        out_specs=(vmem_spec,) * 3,
        scratch_shapes=[
            pltpu.VMEM((seqs, rows, wide), jnp.bfloat16),
            pltpu.VMEM((seqs, 2, pre_rows, width), jnp.bfloat16),
            pltpu.VMEM((seqs, 2, rows, width), jnp.bfloat16),
            pltpu.VMEM((OWNERS, rows, WIDTH), jnp.bfloat16),
            pltpu.VMEM((2, members * pre_rows, DH), jnp.bfloat16),
            pltpu.VMEM((2, members * rows, DH), jnp.bfloat16),
            pltpu.VMEM((OWNERS, rows, WIDTH), jnp.bfloat16),
            pltpu.VMEM((GROUP * rows, members * (pre_rows + rows)), jnp.float32),
            dma((5,)),
        ]
        + [dma((OWNERS,))] * 12
        + [dma((3,)), pltpu.SemaphoreType.REGULAR((2, NZ // 2))],
        compiler_params=pltpu.CompilerParams(
            collective_id=0, has_side_effects=True, vmem_limit_bytes=56 * 2**20
        ),
        name="attend",
    )(prefix_len, queries, stretch_keys, stretch_values, cache_keys, cache_values)
    held = [pltpu.with_memory_space_constraint(array, pltpu.VMEM) for array in held]
    return pl.pallas_call(
        put_out,
        out_shape=tuple(jax.ShapeDtypeStruct(shape, jnp.bfloat16) for shape in shapes),
        in_specs=[vmem_spec] * 3,
        out_specs=(any_spec,) * 3,
        scratch_shapes=[dma((3,))],
        name="put_out",
    )(*held)

def solution(mesh):
    spec = P("grp", "seq", None)
    return jax.shard_map(
        on_device,
        mesh=mesh,
        in_specs=(spec, spec, spec, spec, spec, P("grp")),
        out_specs=(spec, spec, spec),
        check_vma=False,
    )
```

```python
import functools
import math

import jax
import jax.numpy as jnp
from jax import lax
from jax.experimental import pallas as pl
from jax.experimental.pallas import tpu as pltpu
from jax.sharding import PartitionSpec as P

MESH = pl.DeviceIdType.MESH
DH = 128
PAGE = 16
GROUP = 8
WIDTH = GROUP * DH
NZ = 8
NX = 2
OWNERS = NX * NZ
CHUNK = 256
DEAD = -1e30
FACTOR = math.log2(math.e) / math.sqrt(DH)


def offset_of(k):
    t = k // 2
    half = (t + 1) // 2
    return k % 2, half * (1 - 2 * ((t + 1) % 2))


def kernel(
    plen_ref, q_hbm, sk_hbm, sv_hbm, ck_hbm, cv_hbm,
    out_ref, pb_ref, sb_ref,
    q_st, c_st, s_st, q_in, c_in, s_in, o_st, scores,
    load_sem, c_send, c_recv, s_send, s_recv, q_send, q_recv, o_send, o_recv,
    fc_send, fc_recv, fs_send, fs_recv, own_sem, chain,
):
    grp = lax.axis_index("grp")
    seq = lax.axis_index("seq")
    x, z, core = seq // (2 * NZ), (seq // 2) % NZ, seq % 2
    rows = q_hbm.shape[1]
    pre_rows = ck_hbm.shape[1]

    def place(px, pz, pc):
        return (px % NX) * (2 * NZ) + ((pz + NZ) % NZ) * 2 + pc

    def target(k):
        dx, dz = offset_of(k)
        return (x + dx) % NX, (z + dz + NZ) % NZ

    def origin(k):
        dx, dz = offset_of(k)
        return (x + dx) % NX, (z - dz + NZ) % NZ

    loads = [
        pltpu.make_async_copy(ck_hbm, c_st.at[:, 0], load_sem.at[0]),
        pltpu.make_async_copy(cv_hbm, c_st.at[:, 1], load_sem.at[1]),
        pltpu.make_async_copy(sk_hbm, s_st.at[:, 0], load_sem.at[2]),
        pltpu.make_async_copy(sv_hbm, s_st.at[:, 1], load_sem.at[3]),
        pltpu.make_async_copy(q_hbm, q_st, load_sem.at[4]),
    ]

    partner = (grp, place(x, z, 1 - core))
    above, below = (grp, place(x, z + 1, core)), (grp, place(x, z - 1, core))
    across = (grp, place(x + 1, z, core))
    barrier = pltpu.get_barrier_semaphore()
    for near in (above, below, across, partner):
        pl.semaphore_signal(barrier, inc=1, device_id=near, device_id_type=MESH)

    for copy in loads:
        copy.start()

    def tell(level):
        pl.semaphore_signal(chain.at[0, level], inc=1, device_id=above, device_id_type=MESH)
        pl.semaphore_signal(chain.at[1, level], inc=1, device_id=below, device_id_type=MESH)

    def hear(level):
        pl.semaphore_wait(chain.at[0, level], 1)
        pl.semaphore_wait(chain.at[1, level], 1)

    def cols(g, width):
        return pl.ds(pl.multiple_of(g * width, width), width)

    def c_rows(i):
        return pl.ds(pl.multiple_of(i * pre_rows, pre_rows), pre_rows)

    def s_rows(i):
        return pl.ds(pl.multiple_of(i * rows, rows), rows)

    def c_copy(k):
        tx, tz = target(k)
        return pltpu.make_async_remote_copy(
            src_ref=c_st.at[tx, :, :, cols(tz, DH)], dst_ref=c_in.at[:, c_rows(seq)],
            send_sem=c_send.at[k], recv_sem=c_recv.at[k],
            device_id=(grp, place(tx, tz, core)), device_id_type=MESH,
        )

    def s_copy(k):
        tx, tz = target(k)
        return pltpu.make_async_remote_copy(
            src_ref=s_st.at[tx, :, :, cols(tz, DH)], dst_ref=s_in.at[:, s_rows(seq)],
            send_sem=s_send.at[k], recv_sem=s_recv.at[k],
            device_id=(grp, place(tx, tz, core)), device_id_type=MESH,
        )

    def q_copy(k):
        tx, tz = target(k)
        return pltpu.make_async_remote_copy(
            src_ref=q_st.at[tx, :, cols(tz, WIDTH)], dst_ref=q_in.at[k],
            send_sem=q_send.at[k], recv_sem=q_recv.at[k],
            device_id=(grp, place(tx, tz, core)), device_id_type=MESH,
        )

    def o_copy(k):
        ox, oz = origin(k)
        return pltpu.make_async_remote_copy(
            src_ref=o_st.at[k], dst_ref=out_ref.at[x, :, cols(z, WIDTH)],
            send_sem=o_send.at[k], recv_sem=o_recv.at[k],
            device_id=(grp, place(ox, oz, core)), device_id_type=MESH,
        )

    def forward(k):
        ox, oz = origin(k)
        i = place(ox, oz, core)
        return (
            pltpu.make_async_remote_copy(
                src_ref=c_in.at[:, c_rows(i)], dst_ref=c_in.at[:, c_rows(i)],
                send_sem=fc_send.at[k], recv_sem=fc_recv.at[k],
                device_id=partner, device_id_type=MESH,
            ),
            pltpu.make_async_remote_copy(
                src_ref=s_in.at[:, s_rows(i)], dst_ref=s_in.at[:, s_rows(i)],
                send_sem=fs_send.at[k], recv_sem=fs_recv.at[k],
                device_id=partner, device_id_type=MESH,
            ),
        )

    def give(*partners):
        for k in partners:
            c_copy(k).start()
            s_copy(k).start()

    pl.semaphore_wait(barrier, 4)
    tell(0)
    for copy in loads[:4]:
        copy.wait()
    give(2, 4)
    hear(0)
    tell(1)
    give(6, 8, 3, 5)
    hear(1)
    tell(2)
    give(10, 12, 7, 9)
    hear(2)
    tell(3)
    give(14, 11, 13)
    hear(3)
    give(15, 1)
    loads[4].wait()
    for k in reversed(range(1, OWNERS)):
        q_copy(k).start()

    own = [
        pltpu.make_async_copy(c_st.at[x, :, :, cols(z, DH)], c_in.at[:, c_rows(seq)], own_sem.at[0]),
        pltpu.make_async_copy(s_st.at[x, :, :, cols(z, DH)], s_in.at[:, s_rows(seq)], own_sem.at[1]),
        pltpu.make_async_copy(q_st.at[x, :, cols(z, WIDTH)], q_in.at[0], own_sem.at[2]),
    ]
    for copy in own:
        copy.start()

    page0 = seq * (pre_rows // PAGE)

    def bounds(held, s, pages):
        lows, highs = [], []
        for p in range(pages):
            page = held[s, 0, p * PAGE:(p + 1) * PAGE, :].astype(jnp.float32)
            lows.append(jnp.min(page, axis=0, keepdims=True))
            highs.append(jnp.max(page, axis=0, keepdims=True))
        return jnp.concatenate(
            [jnp.concatenate(lows, axis=0), jnp.concatenate(highs, axis=0)], axis=1
        )

    for s in range(c_st.shape[0]):
        pages = pre_rows // PAGE
        both = bounds(c_st, s, pages)
        page = page0 + lax.broadcasted_iota(jnp.int32, both.shape, 0)
        pb_ref[s] = jnp.where(page * PAGE < plen_ref[s], both, 0.0).astype(jnp.bfloat16)
        sb_ref[s] = bounds(s_st, s, rows // PAGE).astype(jnp.bfloat16)

    for copy in own:
        copy.wait()
    for k in range(OWNERS):
        if k:
            c_copy(k).wait_recv()
            s_copy(k).wait_recv()
        for copy in forward(k):
            copy.start()
    for k in range(OWNERS):
        for copy in forward(k):
            copy.wait_recv()

    length = plen_ref[x]
    block_rows = GROUP * rows
    n_pre = c_in.shape[1] // CHUNK
    n_new = s_in.shape[1] // CHUNK

    def attend(k):
        ox, oz = origin(k)
        first = place(ox, oz, core) * rows
        q = jnp.concatenate([q_in[k, :, h * DH:(h + 1) * DH] for h in range(GROUP)], axis=0)
        lane = lax.broadcasted_iota(jnp.int32, (1, CHUNK), 1)
        row = first + lax.broadcasted_iota(jnp.int32, (block_rows, 1), 0) % rows
        top = jnp.full((block_rows, DH), DEAD, jnp.float32)
        for j in range(n_pre + n_new):
            if j < n_pre:
                key = c_in[0, j * CHUNK:(j + 1) * CHUNK, :]
                live = lane + j * CHUNK < length
            else:
                key = s_in[0, (j - n_pre) * CHUNK:(j - n_pre + 1) * CHUNK, :]
                live = lane + (j - n_pre) * CHUNK <= row
            s = lax.dot_general(
                q, key, (((1,), (1,)), ((), ())), preferred_element_type=jnp.float32
            )
            s = jnp.where(live, s, DEAD)
            scores[:, j * CHUNK:(j + 1) * CHUNK] = s
            for i in range(CHUNK // DH):
                top = jnp.maximum(top, s[:, i * DH:(i + 1) * DH])
        top = jnp.max(top, axis=1, keepdims=True)
        total = jnp.zeros((block_rows, DH), jnp.float32)
        acc = jnp.zeros((block_rows, DH), jnp.float32)
        for j in range(n_pre + n_new):
            if j < n_pre:
                value = c_in[1, j * CHUNK:(j + 1) * CHUNK, :]
            else:
                value = s_in[1, (j - n_pre) * CHUNK:(j - n_pre + 1) * CHUNK, :]
            w = jnp.exp2((scores[:, j * CHUNK:(j + 1) * CHUNK] - top) * FACTOR)
            for i in range(CHUNK // DH):
                total = total + w[:, i * DH:(i + 1) * DH]
            acc = acc + jnp.dot(
                w.astype(jnp.bfloat16), value, preferred_element_type=jnp.float32
            )
        out = (acc / jnp.sum(total, axis=1, keepdims=True)).astype(jnp.bfloat16)
        for h in range(GROUP):
            o_st[k, :, h * DH:(h + 1) * DH] = out[h * rows:(h + 1) * rows, :]

    def step(i, carry):
        k = OWNERS - 1 - i
        q_copy(k).wait_recv()
        attend(k)

        @pl.when(i > 0)
        def _():
            o_copy(k + 1).start()

        return carry

    lax.fori_loop(0, OWNERS - 1, step, 0)
    attend(0)
    o_copy(1).start()
    mine = pltpu.make_async_copy(o_st.at[0], out_ref.at[x, :, cols(z, WIDTH)], own_sem.at[0])

    for k in range(1, OWNERS):
        c_copy(k).wait_send()
        s_copy(k).wait_send()
        q_copy(k).wait_send()
    for k in range(OWNERS):
        for copy in forward(k):
            copy.wait_send()
    mine.start()
    for k in range(1, OWNERS):
        o_copy(k).wait()
    mine.wait()


def put_out(*refs):
    *ends, sem = refs
    half = len(ends) // 2
    copies = [pltpu.make_async_copy(ends[i], ends[half + i], sem.at[i]) for i in range(half)]
    for copy in copies:
        copy.start()
    for copy in copies:
        copy.wait()


def on_device(queries, stretch_keys, stretch_values, cache_keys, cache_values, prefix_len):
    seqs, rows, wide = queries.shape
    pre_rows, width = cache_keys.shape[1:]
    members = lax.axis_size("seq")
    dma = pltpu.SemaphoreType.DMA
    any_spec = pl.BlockSpec(memory_space=pl.ANY)
    vmem_spec = pl.BlockSpec(memory_space=pltpu.VMEM)
    shapes = (
        (seqs, rows, wide),
        (seqs, pre_rows // PAGE, 2 * width),
        (seqs, rows // PAGE, 2 * width),
    )
    held = pl.pallas_call(
        kernel,
        out_shape=tuple(pltpu.VMEM(shape, jnp.bfloat16) for shape in shapes),
        in_specs=[pl.BlockSpec(memory_space=pltpu.SMEM)] + [any_spec] * 5,
        out_specs=(vmem_spec,) * 3,
        scratch_shapes=[
            pltpu.VMEM((seqs, rows, wide), jnp.bfloat16),
            pltpu.VMEM((seqs, 2, pre_rows, width), jnp.bfloat16),
            pltpu.VMEM((seqs, 2, rows, width), jnp.bfloat16),
            pltpu.VMEM((OWNERS, rows, WIDTH), jnp.bfloat16),
            pltpu.VMEM((2, members * pre_rows, DH), jnp.bfloat16),
            pltpu.VMEM((2, members * rows, DH), jnp.bfloat16),
            pltpu.VMEM((OWNERS, rows, WIDTH), jnp.bfloat16),
            pltpu.VMEM((GROUP * rows, members * (pre_rows + rows)), jnp.float32),
            dma((5,)),
        ]
        + [dma((OWNERS,))] * 12
        + [dma((3,)), pltpu.SemaphoreType.REGULAR((2, NZ // 2))],
        compiler_params=pltpu.CompilerParams(
            collective_id=0, has_side_effects=True, vmem_limit_bytes=56 * 2**20
        ),
        name="attend",
    )(prefix_len, queries, stretch_keys, stretch_values, cache_keys, cache_values)
    held = [pltpu.with_memory_space_constraint(array, pltpu.VMEM) for array in held]
    return pl.pallas_call(
        put_out,
        out_shape=tuple(jax.ShapeDtypeStruct(shape, jnp.bfloat16) for shape in shapes),
        in_specs=[vmem_spec] * 3,
        out_specs=(any_spec,) * 3,
        scratch_shapes=[dma((3,))],
        name="put_out",
    )(*held)

def solution(mesh):
    spec = P("grp", "seq", None)
    return jax.shard_map(
        on_device,
        mesh=mesh,
        in_specs=(spec, spec, spec, spec, spec, P("grp")),
        out_specs=(spec, spec, spec),
        check_vma=False,
    )
```
